128 devices in a mesh: layer: 4 (over x), col: 32 (over z, y, core).
Axes of the slice: x: 4, y: 4, z: 4, core: 2. Of those that a mesh axis runs over, the one named last changes fastest.
Arguments:
- inputs: bfloat16 [4, 128, 4096], replicated, may hold values from -6 to 6
- w_input: bfloat16 [4, 4096, 4, 4096], P('layer', None, None, 'col'), may hold values from -0.09375 to 0.09375
- w_recur: bfloat16 [4, 4096, 4, 4096], P('layer', None, None, 'col'), may hold values from -0.09375 to 0.09375
- bias: float32 [4, 4, 4096], P('layer', None, 'col'), may hold values from -1 to 2
- h_start: bfloat16 [4, 128, 4096], P('layer', None, 'col'), may hold values from -3 to 3
- c_start: float32 [4, 128, 4096], P('layer', None, 'col'), may hold values from -6 to 6
Outputs:
- hidden_seq: bfloat16 [4, 4, 128, 4096], P('layer', None, None, 'col')
- cell_final: float32 [4, 128, 4096], P('layer', None, 'col')
The draws below stay inside these ranges and needn't reach their ends.
All inputs are finite; a program needn't handle non-finite values.
Results may differ from the reference program's by a relative error of at most 0.0024.
Values may be sent and summed in bfloat16 or wider, within the bound.
No kernel may reach another device: no remote copies, remote signals or barrier semaphores. Data moves between devices by JAX's collectives and lax.ppermute only.
A program may use at most 64 MiB of HBM per device.

```python
import jax
import jax.numpy as jnp
from jax import lax

H = 4096
BATCH = 128
TSTEPS = 4
LAYERS = 4


def steps_of(rng, extent, cuts, smallest, high):
    loudness, own = 1.0, jax.random.fold_in(rng, 6)
    for dim, shards_of in cuts:
        heights = jnp.exp(jax.random.uniform(jax.random.fold_in(own, dim), (shards_of,), jnp.float32, smallest / len(cuts), high / len(cuts)))
        loudness = loudness * jnp.repeat(heights, extent[dim] // shards_of).reshape([-1 if axis == dim else 1 for axis in range(len(extent))])
    return loudness


def scatter_about(own_key, dims, width, limit, split=(), held_as=jnp.bfloat16):
    entries = jax.random.normal(own_key, dims, jnp.float32) * width
    if len(split) > 0:
        entries = steps_of(own_key, dims, split, -0.22, 0.18) * entries
    return jnp.clip(entries, min=-limit, max=limit).astype(held_as)


def setup_inputs(seed: int = 0) -> dict:
    seeds = jax.random.split(jax.random.key(seed), 7)
    inputs = scatter_about(seeds[0], (TSTEPS, BATCH, H), 1.0, 6.0)
    w_input = scatter_about(seeds[1], (LAYERS, H, 4, H), H ** -0.5, 0.09375, ((0, 4), (3, 32)))
    w_recur = scatter_about(seeds[2], (LAYERS, H, 4, H), H ** -0.5, 0.09375, ((0, 4), (3, 32)))
    bias = jnp.clip(-1.0 + 3.0 * jax.random.uniform(seeds[3], (LAYERS, 4, H), jnp.float32) ** steps_of(seeds[3], (LAYERS, 4, H), ((0, 4), (2, 32)), -0.2, 0.2), -1.0, 2.0)
    h_start = scatter_about(seeds[4], (LAYERS, BATCH, H), 0.5, 3.0, ((0, 4), (2, 32)))
    c_start = scatter_about(seeds[5], (LAYERS, BATCH, H), 1.0, 6.0, ((0, 4), (2, 32)), jnp.float32)
    return {"inputs": inputs, "w_input": w_input, "w_recur": w_recur, "bias": bias, "h_start": h_start, "c_start": c_start}


def reference(inputs, w_input, w_recur, bias, h_start, c_start):
    layers = w_input.shape[0]
    source = inputs
    hidden_all = []
    cell_all = []
    for layer in range(layers):
        weight_in = w_input[layer].reshape(H, 4 * H)
        weight_rec = w_recur[layer].reshape(H, 4 * H)
        offset = bias[layer].reshape(4 * H)
        projected = jnp.dot(source.reshape(TSTEPS * BATCH, H), weight_in, preferred_element_type=jnp.float32) + offset
        projected = projected.reshape(TSTEPS, BATCH, 4 * H)

        def advance(carry, z_in, weight_rec=weight_rec):
            hidden, cell = carry
            gates = z_in + jnp.dot(hidden, weight_rec, preferred_element_type=jnp.float32)
            gates = gates.reshape(BATCH, 4, H)
            cell_new = jax.nn.sigmoid(gates[:, 1]) * cell + jax.nn.sigmoid(gates[:, 0]) * jnp.tanh(gates[:, 2])
            hidden_new = (jax.nn.sigmoid(gates[:, 3]) * jnp.tanh(cell_new)).astype(jnp.bfloat16)
            return (hidden_new, cell_new), hidden_new

        (hidden_last, cell_last), outputs = lax.scan(advance, (h_start[layer], c_start[layer]), projected)
        hidden_all.append(outputs)
        cell_all.append(cell_last)
        source = outputs
    return jnp.stack(hidden_all), jnp.stack(cell_all)
```

```python
import functools

import jax
import jax.numpy as jnp
from jax import lax
from jax.experimental import pallas as pl
from jax.experimental.pallas import tpu as pltpu
from jax.sharding import PartitionSpec as P


def in_vmem(count):
    return [pl.BlockSpec(memory_space=pltpu.VMEM)] * count


def product_kernel(depth, g_ref, w_ref, out_ref):
    blocks = g_ref.shape[0]
    wide = 256
    for n in range(out_ref.shape[1] // wide):
        cols = slice(n * wide, (n + 1) * wide)
        total = None
        for j in range(blocks):
            term = jnp.dot(
                g_ref[j], w_ref[j, :depth, cols], preferred_element_type=jnp.float32
            )
            total = term if total is None else total + term
        out_ref[:, cols] = total


def product(g, w):
    blocks, rows, depth = g.shape
    width = w.shape[2]
    return pl.pallas_call(
        functools.partial(product_kernel, depth),
        out_shape=jax.ShapeDtypeStruct((rows, width), jnp.float32),
        in_specs=in_vmem(2),
        out_specs=pl.BlockSpec(memory_space=pltpu.VMEM),
        cost_estimate=pl.CostEstimate(
            flops=2 * blocks * rows * depth * width,
            bytes_accessed=2 * blocks * depth * (rows + width) + 4 * rows * width,
            transcendentals=0,
        ),
        compiler_params=pltpu.CompilerParams(vmem_limit_bytes=16 << 20),
    )(g, w)


def body(inputs, w_input, w_recur, bias, h_start, c_start):
    steps, batch, width = inputs.shape
    unit = w_input.shape[3]
    layers = lax.axis_size("layer")
    devices = lax.axis_size("col")
    chips = devices // 2
    turns = steps + layers - 1
    layer = lax.axis_index("layer")
    core = lax.axis_index("col") % 2
    same_core = [[2 * chip + side for chip in range(chips)] for side in range(2)]
    partners = [(i, i ^ 1) for i in range(devices)]
    upward = [(i, i + 1) for i in range(layers - 1)]

    def across(x):
        return lax.ppermute(x, "col", partners)

    def gathered(x):
        copies = jnp.broadcast_to(x, (chips, *x.shape))
        return lax.all_to_all(copies, "col", 0, 0, tiled=True, axis_index_groups=same_core)

    start = gathered(h_start[0])

    def halves(w):
        w = w[0].reshape(chips, 2, unit, 4 * unit)
        keep = lax.dynamic_index_in_dim(w, core, 1, keepdims=False)
        away = lax.dynamic_index_in_dim(w, 1 - core, 1, keepdims=False)
        return keep, across(away)

    rec_keep, rec_send = halves(w_recur)
    in_keep, in_send = halves(w_input)
    w_keep = jnp.concatenate([rec_keep, in_keep], axis=1)
    w_send = jnp.concatenate([rec_send, in_send], axis=1)
    first = jnp.dot(
        inputs.reshape(steps * batch, width),
        w_input[0].reshape(width, 4 * unit),
        preferred_element_type=jnp.float32,
    ).reshape(steps, batch, 4 * unit)
    offset = bias[0].reshape(4 * unit)

    cell = c_start[0]
    hidden = h_start[0]
    kept = []
    blocks = start
    for turn in range(turns):
        leaving = across(product(blocks, w_send))
        staying = product(blocks, w_keep)
        z = staying + leaving + offset
        if turn < steps:
            z = z + jnp.where(layer == 0, first[turn], 0.0)
        i, f, g, o = (z[:, k * unit : (k + 1) * unit] for k in range(4))
        cell_new = jax.nn.sigmoid(f) * cell + jax.nn.sigmoid(i) * jnp.tanh(g)
        hidden_new = (jax.nn.sigmoid(o) * jnp.tanh(cell_new)).astype(jnp.bfloat16)
        valid = jnp.logical_and(turn >= layer, turn < layer + steps)
        cell = jnp.where(valid, cell_new, cell)
        hidden = jnp.where(valid, hidden_new, hidden)
        kept.append(hidden)
        if turn + 1 < turns:
            below = lax.ppermute(hidden, "layer", upward)
            blocks = gathered(jnp.concatenate([hidden, below], axis=1))
    sequence = lax.dynamic_slice_in_dim(jnp.stack(kept), layer, steps, 0)
    return sequence[None], cell[None]


def solution(mesh):
    in_specs = (
        P(),
        P("layer", None, None, "col"),
        P("layer", None, None, "col"),
        P("layer", None, "col"),
        P("layer", None, "col"),
        P("layer", None, "col"),
    )
    out_specs = (P("layer", None, None, "col"), P("layer", None, "col"))
    return jax.shard_map(body, mesh=mesh, in_specs=in_specs, out_specs=out_specs, check_vma=False)
```

```python
import functools

import jax
import jax.numpy as jnp
from jax import lax
from jax.experimental import pallas as pl
from jax.experimental.pallas import tpu as pltpu
from jax.sharding import PartitionSpec as P

VMEM = pl.BlockSpec(memory_space=pltpu.VMEM)
SMEM = pl.BlockSpec(memory_space=pltpu.SMEM)
ANY = pl.BlockSpec(memory_space=pl.ANY)


def resident(x):
    return pltpu.with_memory_space_constraint(x, pltpu.VMEM)


def limits(mib):
    return pltpu.CompilerParams(vmem_limit_bytes=mib << 20)


def sort_kernel(other, info_ref, w_ref, out_ref):
    blocks, depth, wide = out_ref.shape
    unit = w_ref.shape[1]
    gates = wide // unit
    half = depth // 2
    rows = half * gates
    side = 1 - info_ref[1] if other else info_ref[1]
    to = lax.broadcasted_iota(jnp.int32, (rows, rows), 0)
    come = lax.broadcasted_iota(jnp.int32, (rows, rows), 1)
    order = come == gates * (to % half) + to // half
    order = order.astype(jnp.float32).astype(jnp.bfloat16)
    unroll = 8

    def some(i, carry):
        for u in range(unroll):
            j = i * unroll + u
            at = pl.multiple_of((2 * j + side) * 2 * rows, 2 * rows)
            both = jnp.concatenate(
                [w_ref[pl.ds(at, rows), :], w_ref[pl.ds(at + rows, rows), :]], axis=1
            )
            sorted_rows = jnp.dot(order, both, preferred_element_type=jnp.float32)
            sorted_rows = sorted_rows.astype(jnp.bfloat16)
            for h in range(2):
                for g in range(gates):
                    out_ref[j, h * half : (h + 1) * half, g * unit : (g + 1) * unit] = sorted_rows[
                        g * half : (g + 1) * half, h * unit : (h + 1) * unit
                    ]
        return carry

    lax.fori_loop(0, blocks // unroll, some, 0)


def sorted_side(info, w, blocks, other):
    depth, gates, unit = w.shape[0] // (2 * blocks), w.shape[1], w.shape[2]
    return pl.pallas_call(
        functools.partial(sort_kernel, other),
        out_shape=jax.ShapeDtypeStruct((blocks, depth, gates * unit), w.dtype),
        in_specs=[SMEM, VMEM],
        out_specs=VMEM,
        cost_estimate=pl.CostEstimate(
            flops=2_000_000_000, bytes_accessed=4 * blocks * depth * gates * unit, transcendentals=0
        ),
        compiler_params=limits(4),
    )(info, resident(w.reshape(-1, unit)))


def pick_kernel(info_ref, x_ref, out_ref, sems):
    blocks, unit = out_ref.shape[1], out_ref.shape[3]
    copies = []
    for j in range(blocks):
        at = pl.multiple_of((2 * j + info_ref[1]) * unit, unit)
        copies.append(
            pltpu.make_async_copy(x_ref.at[:, :, pl.ds(at, unit)], out_ref.at[:, j], sems.at[j])
        )
    for copy in copies:
        copy.start()
    for copy in copies:
        copy.wait()


def picked(info, x, blocks, unit):
    steps, batch, _ = x.shape
    return pl.pallas_call(
        pick_kernel,
        out_shape=jax.ShapeDtypeStruct((steps, blocks, batch, unit), x.dtype),
        in_specs=[SMEM, ANY],
        out_specs=VMEM,
        scratch_shapes=[pltpu.SemaphoreType.DMA((blocks,))],
        cost_estimate=pl.CostEstimate(
            flops=1_000_000_000, bytes_accessed=4 * x.size // 2, transcendentals=0
        ),
        compiler_params=limits(1),
    )(info, x)


def product_kernel(turn, stage, fed, info_ref, *refs):
    refs = list(refs)
    out_ref, w_in_ref, w_rec_ref = refs.pop(), refs.pop(), refs.pop()
    x_ref = refs.pop() if fed else None
    blocks, unit, width = w_rec_ref.shape
    bottom = info_ref[0] == 0

    def own(j):
        if stage == 0:
            return refs[0][j]
        if stage == 1:
            return jnp.where(bottom, refs[1][j], refs[0][j])
        return refs[0][j, :, :unit]

    def below(j):
        if stage == 0:
            came = jnp.zeros_like(x_ref[turn, j])
        elif stage == 1:
            came = refs[1][j]
        else:
            came = refs[0][j, :, unit:]
        return jnp.where(bottom, x_ref[turn, j], came) if fed else came

    wide = 256
    for n in range(width // wide):
        cols = slice(n * wide, (n + 1) * wide)
        total = None
        for block, w_ref in ((own, w_rec_ref), (below, w_in_ref)):
            for j in range(0, blocks, 2):
                left = jnp.concatenate([block(j), block(j + 1)], axis=1)
                right = w_ref[j : j + 2, :, cols].reshape(2 * unit, wide)
                term = jnp.dot(left, right, preferred_element_type=jnp.float32)
                total = term if total is None else total + term
        out_ref[:, cols] = total


def product(info, gathered, x, w_rec, w_in, turn, stage):
    blocks, unit, width = w_rec.shape
    batch = gathered[0].shape[1]
    args = [*gathered, *([] if x is None else [x]), w_rec, w_in]
    return pl.pallas_call(
        functools.partial(product_kernel, turn, stage, x is not None),
        out_shape=jax.ShapeDtypeStruct((batch, width), jnp.float32),
        in_specs=[SMEM, *[VMEM] * len(args)],
        out_specs=VMEM,
        cost_estimate=pl.CostEstimate(
            flops=4 * blocks * unit * batch * width,
            bytes_accessed=4 * blocks * unit * (batch + width) + 4 * batch * width,
            transcendentals=0,
        ),
        compiler_params=limits(4),
    )(info, *[resident(arg) for arg in args])


def gates_kernel(turn, steps, info_ref, here_ref, came_ref, bias_ref, cell_ref, hid_ref, cell_out, hid_out):
    unit = cell_ref.shape[1]
    layer = info_ref[0]
    valid = jnp.logical_and(turn >= layer, turn < layer + steps)

    def gate(k):
        cols = slice(k * unit, (k + 1) * unit)
        return here_ref[:, cols] + came_ref[:, cols] + bias_ref[k : k + 1, :]

    cell = cell_ref[...]
    cell_new = jax.nn.sigmoid(gate(1)) * cell + jax.nn.sigmoid(gate(0)) * jnp.tanh(gate(2))
    hidden_new = (jax.nn.sigmoid(gate(3)) * jnp.tanh(cell_new)).astype(hid_ref.dtype)
    cell_out[...] = jnp.where(valid, cell_new, cell)
    hid_out[...] = jnp.where(valid, hidden_new, hid_ref[...])


def gates(info, here, came, bias, cell, hidden, turn, steps):
    return pl.pallas_call(
        functools.partial(gates_kernel, turn, steps),
        out_shape=(
            jax.ShapeDtypeStruct(cell.shape, cell.dtype),
            jax.ShapeDtypeStruct(hidden.shape, hidden.dtype),
        ),
        in_specs=[SMEM, *[VMEM] * 5],
        out_specs=(VMEM, VMEM),
        cost_estimate=pl.CostEstimate(
            flops=20 * cell.size, bytes_accessed=40 * cell.size, transcendentals=5 * cell.size
        ),
        compiler_params=limits(2),
    )(info, *[resident(arg) for arg in (here, came, bias, cell, hidden)])


def spread_kernel(stage, info_ref, *refs):
    out_ref = refs[-1]
    unit = refs[0].shape[1]
    for j in range(out_ref.shape[0]):
        if stage == 0:
            out_ref[j] = refs[0][...]
        elif stage == 1:
            out_ref[j] = jnp.where(info_ref[0] == 0, refs[0][...], refs[1][...])
        else:
            out_ref[j, :, :unit] = refs[0][...]
            out_ref[j, :, unit:] = refs[1][...]


def spread(info, parts, stage, copies):
    batch, unit = parts[0].shape
    width = unit * (2 if stage == 2 else 1)
    return pl.pallas_call(
        functools.partial(spread_kernel, stage),
        out_shape=jax.ShapeDtypeStruct((copies, batch, width), parts[0].dtype),
        in_specs=[SMEM, *[VMEM] * len(parts)],
        out_specs=VMEM,
        cost_estimate=pl.CostEstimate(
            flops=batch * width, bytes_accessed=2 * copies * batch * width, transcendentals=0
        ),
        compiler_params=limits(2),
    )(info, *[resident(part) for part in parts])


def select_kernel(layers, info_ref, *refs):
    out_ref = refs[-1]
    for t in range(out_ref.shape[0]):
        value = refs[t][...]
        for l in range(1, layers):
            value = jnp.where(info_ref[0] == l, refs[t + l][...], value)
        out_ref[t] = value


def selected(info, kept, steps, layers):
    return pl.pallas_call(
        functools.partial(select_kernel, layers),
        out_shape=jax.ShapeDtypeStruct((steps, *kept[0].shape), kept[0].dtype),
        in_specs=[SMEM, *[VMEM] * len(kept)],
        out_specs=VMEM,
        compiler_params=limits(2),
    )(info, *[resident(value) for value in kept])


def body(inputs, w_input, w_recur, bias, h_start, c_start):
    steps, _, _ = inputs.shape
    unit = w_input.shape[3]
    layers = lax.axis_size("layer")
    devices = lax.axis_size("col")
    chips = devices // 2
    turns = steps + layers - 1
    layer = lax.axis_index("layer")
    core = lax.axis_index("col") & 1
    same_core = [[2 * chip + side for chip in range(chips)] for side in range(2)]
    partners = [(i, i ^ 1) for i in range(devices)]
    upward = [(i, i + 1) for i in range(layers - 1)]
    info = jnp.stack([layer, core])

    def across(x):
        return lax.ppermute(x, "col", partners)

    def gathered(parts, stage):
        copies = spread(info, parts, stage, chips)
        return lax.all_to_all(copies, "col", 0, 0, tiled=True, axis_index_groups=same_core)

    cell = c_start[0]
    hidden = h_start[0]
    start = gathered((hidden,), 0)
    rec_send = across(sorted_side(info, w_recur[0], chips, True))
    in_send = across(sorted_side(info, w_input[0], chips, True))
    rec_keep = sorted_side(info, w_recur[0], chips, False)
    in_keep = sorted_side(info, w_input[0], chips, False)
    x = picked(info, inputs, chips, unit)

    kept = []
    blocks = (start,)
    for turn in range(turns):
        stage = min(turn, 2)
        fed = x if turn < steps else None
        came = across(product(info, blocks, fed, rec_send, in_send, turn, stage))
        here = product(info, blocks, fed, rec_keep, in_keep, turn, stage)
        cell, hidden = gates(info, here, came, bias[0], cell, hidden, turn, steps)
        kept.append(hidden)
        if turn + 1 < turns:
            below = lax.ppermute(hidden, "layer", upward)
            blocks = (gathered((hidden, below), min(turn + 1, 2)),)
            if turn == 0:
                blocks = (start, *blocks)
    return selected(info, kept, steps, layers)[None], cell[None]


def solution(mesh):
    in_specs = (
        P(),
        P("layer", None, None, "col"),
        P("layer", None, None, "col"),
        P("layer", None, "col"),
        P("layer", None, "col"),
        P("layer", None, "col"),
    )
    out_specs = (P("layer", None, None, "col"), P("layer", None, "col"))
    return jax.shard_map(body, mesh=mesh, in_specs=in_specs, out_specs=out_specs, check_vma=False)
```

```python
import functools

import jax
import jax.numpy as jnp
from jax import lax
from jax.experimental import pallas as pl
from jax.experimental.pallas import tpu as pltpu
from jax.sharding import PartitionSpec as P

VMEM = pl.BlockSpec(memory_space=pltpu.VMEM)
HBM = pl.BlockSpec(memory_space=pltpu.HBM)


def resident(x):
    return pltpu.with_memory_space_constraint(x, pltpu.VMEM)


def outside(x):
    return pltpu.with_memory_space_constraint(x, pltpu.HBM)


def limits(mib):
    return pltpu.CompilerParams(vmem_limit_bytes=mib << 20)


def sort_kernel(other, w_ref, out_ref, natural, ordered, in_sems, out_sems):
    blocks, depth, wide = ordered.shape
    unit = natural.shape[2]
    gates = wide // unit
    half = depth // 2
    rows = half * gates
    core = lax.axis_index("col") & 1
    side = 1 - core if other else core
    to = lax.broadcasted_iota(jnp.int32, (rows, rows), 0)
    come = lax.broadcasted_iota(jnp.int32, (rows, rows), 1)
    order = come == gates * (to % half) + to // half
    order = order.astype(jnp.float32).astype(jnp.bfloat16)
    parts = in_sems.shape[0]
    size = blocks // parts

    def incoming(part):
        chosen = pl.ds(part * size, size)
        return pltpu.make_async_copy(w_ref.at[chosen, side], natural.at[chosen], in_sems.at[part])

    def outgoing(part):
        chosen = pl.ds(part * size, size)
        return pltpu.make_async_copy(ordered.at[chosen], out_ref.at[chosen], out_sems.at[part])

    for part in range(parts):
        incoming(part).start()
    for part in range(parts):
        incoming(part).wait()
        for j in range(part * size, (part + 1) * size):
            both = jnp.concatenate([natural[j, :rows, :], natural[j, rows:, :]], axis=1)
            sorted_rows = jnp.dot(order, both, preferred_element_type=jnp.float32)
            sorted_rows = sorted_rows.astype(jnp.bfloat16)
            for h in range(2):
                for g in range(gates):
                    ordered[j, h * half : (h + 1) * half, g * unit : (g + 1) * unit] = sorted_rows[
                        g * half : (g + 1) * half, h * unit : (h + 1) * unit
                    ]
        outgoing(part).start()
    for part in range(parts):
        outgoing(part).wait()


def sorted_side(w, blocks, other):
    gates, unit = w.shape[1:]
    depth = w.shape[0] // (2 * blocks)
    wide = gates * unit
    parts = 4
    return pl.pallas_call(
        functools.partial(sort_kernel, other),
        out_shape=pltpu.HBM((blocks, depth, wide), w.dtype),
        in_specs=[HBM],
        out_specs=HBM,
        scratch_shapes=[
            pltpu.VMEM((blocks, depth * gates, unit), w.dtype),
            pltpu.VMEM((blocks, depth, wide), w.dtype),
            pltpu.SemaphoreType.DMA((parts,)),
            pltpu.SemaphoreType.DMA((parts,)),
        ],
        cost_estimate=pl.CostEstimate(
            flops=2_000_000_000, bytes_accessed=4 * blocks * depth * wide, transcendentals=0
        ),
        compiler_params=limits(8),
    )(outside(w.reshape(blocks, 2, depth * gates, unit)))


def pick_kernel(x_ref, out_ref, sems):
    blocks, unit = out_ref.shape[1], out_ref.shape[3]
    core = lax.axis_index("col") & 1
    copies = []
    for j in range(blocks):
        at = pl.multiple_of((2 * j + core) * unit, unit)
        copies.append(
            pltpu.make_async_copy(x_ref.at[:, :, pl.ds(at, unit)], out_ref.at[:, j], sems.at[j])
        )
    for copy in copies:
        copy.start()
    for copy in copies:
        copy.wait()


def picked(x, blocks, unit):
    steps, batch, _ = x.shape
    return pl.pallas_call(
        pick_kernel,
        out_shape=jax.ShapeDtypeStruct((steps, blocks, batch, unit), x.dtype),
        in_specs=[HBM],
        out_specs=VMEM,
        scratch_shapes=[pltpu.SemaphoreType.DMA((blocks,))],
        cost_estimate=pl.CostEstimate(
            flops=1_000_000_000, bytes_accessed=4 * x.size // 2, transcendentals=0
        ),
        compiler_params=limits(1),
    )(outside(x))


def fetch_kernel(count, *refs):
    sems = refs[-1]
    copies = [
        pltpu.make_async_copy(refs[i], refs[count + 1 + i], sems.at[i]) for i in range(count)
    ]
    for copy in copies:
        copy.start()
    for copy in copies:
        copy.wait()


def fetched(arrays, after):
    count = len(arrays)
    return pl.pallas_call(
        functools.partial(fetch_kernel, count),
        out_shape=tuple(jax.ShapeDtypeStruct(array.shape, array.dtype) for array in arrays),
        in_specs=[*[HBM] * count, pl.BlockSpec(memory_space=pl.ANY)],
        out_specs=tuple([VMEM] * count),
        scratch_shapes=[pltpu.SemaphoreType.DMA((count,))],
        compiler_params=limits(1),
    )(*[outside(array) for array in arrays], after)


def product_kernel(turn, stage, fed, *refs):
    refs = list(refs)
    out_ref, w_in_ref, w_rec_ref = refs.pop(), refs.pop(), refs.pop()
    x_ref = refs.pop() if fed else None
    blocks, unit, width = w_rec_ref.shape
    bottom = lax.axis_index("layer") == 0

    def own(j):
        if stage == 0:
            return refs[0][j]
        if stage == 1:
            return jnp.where(bottom, refs[1][j], refs[0][j])
        return refs[0][j, :, :unit]

    def below(j):
        if stage == 0:
            came = jnp.zeros_like(x_ref[turn, j])
        elif stage == 1:
            came = refs[1][j]
        else:
            came = refs[0][j, :, unit:]
        return jnp.where(bottom, x_ref[turn, j], came) if fed else came

    wide = 256
    for n in range(width // wide):
        cols = slice(n * wide, (n + 1) * wide)
        total = None
        for block, w_ref in ((own, w_rec_ref), (below, w_in_ref)):
            for j in range(0, blocks, 2):
                left = jnp.concatenate([block(j), block(j + 1)], axis=1)
                right = w_ref[j : j + 2, :, cols].reshape(2 * unit, wide)
                term = jnp.dot(left, right, preferred_element_type=jnp.float32)
                total = term if total is None else total + term
        out_ref[:, cols] = total


def product(gathered, x, w_rec, w_in, turn, stage):
    blocks, unit, width = w_rec.shape
    batch = gathered[0].shape[1]
    args = [*gathered, *([] if x is None else [x]), w_rec, w_in]
    return pl.pallas_call(
        functools.partial(product_kernel, turn, stage, x is not None),
        out_shape=jax.ShapeDtypeStruct((batch, width), jnp.float32),
        in_specs=[*[VMEM] * len(args)],
        out_specs=VMEM,
        cost_estimate=pl.CostEstimate(
            flops=4 * blocks * unit * batch * width,
            bytes_accessed=4 * blocks * unit * (batch + width) + 4 * batch * width,
            transcendentals=0,
        ),
        compiler_params=limits(4),
    )(*[resident(arg) for arg in args])


def gates_kernel(turn, steps, here_ref, came_ref, bias_ref, cell_ref, hid_ref, cell_out, hid_out):
    unit = cell_ref.shape[1]
    layer = lax.axis_index("layer")
    valid = jnp.logical_and(turn >= layer, turn < layer + steps)

    def gate(k):
        cols = slice(k * unit, (k + 1) * unit)
        return here_ref[:, cols] + came_ref[:, cols] + bias_ref[k : k + 1, :]

    cell = cell_ref[...]
    cell_new = jax.nn.sigmoid(gate(1)) * cell + jax.nn.sigmoid(gate(0)) * jnp.tanh(gate(2))
    hidden_new = (jax.nn.sigmoid(gate(3)) * jnp.tanh(cell_new)).astype(hid_ref.dtype)
    cell_out[...] = jnp.where(valid, cell_new, cell)
    hid_out[...] = jnp.where(valid, hidden_new, hid_ref[...])


def gates(here, came, bias, cell, hidden, turn, steps):
    return pl.pallas_call(
        functools.partial(gates_kernel, turn, steps),
        out_shape=(
            jax.ShapeDtypeStruct(cell.shape, cell.dtype),
            jax.ShapeDtypeStruct(hidden.shape, hidden.dtype),
        ),
        in_specs=[*[VMEM] * 5],
        out_specs=(VMEM, VMEM),
        cost_estimate=pl.CostEstimate(
            flops=20 * cell.size, bytes_accessed=40 * cell.size, transcendentals=5 * cell.size
        ),
        compiler_params=limits(2),
    )(*[resident(arg) for arg in (here, came, bias, cell, hidden)])


def spread_kernel(stage, *refs):
    out_ref = refs[-1]
    unit = refs[0].shape[1]
    layer = lax.axis_index("layer")
    for j in range(out_ref.shape[0]):
        if stage == 0:
            out_ref[j] = refs[0][...]
        elif stage == 1:
            out_ref[j] = jnp.where(layer == 0, refs[0][...], refs[1][...])
        else:
            out_ref[j, :, :unit] = refs[0][...]
            out_ref[j, :, unit:] = refs[1][...]


def spread(parts, stage, copies):
    batch, unit = parts[0].shape
    width = unit * (2 if stage == 2 else 1)
    return pl.pallas_call(
        functools.partial(spread_kernel, stage),
        out_shape=jax.ShapeDtypeStruct((copies, batch, width), parts[0].dtype),
        in_specs=[*[VMEM] * len(parts)],
        out_specs=VMEM,
        cost_estimate=pl.CostEstimate(
            flops=batch * width, bytes_accessed=2 * copies * batch * width, transcendentals=0
        ),
        compiler_params=limits(2),
    )(*[resident(part) for part in parts])


def select_kernel(layers, *refs):
    out_ref = refs[-1]
    layer = lax.axis_index("layer")
    for t in range(out_ref.shape[0]):
        value = refs[t][...]
        for l in range(1, layers):
            value = jnp.where(layer == l, refs[t + l][...], value)
        out_ref[t] = value


def selected(kept, steps, layers):
    return pl.pallas_call(
        functools.partial(select_kernel, layers),
        out_shape=jax.ShapeDtypeStruct((steps, *kept[0].shape), kept[0].dtype),
        in_specs=[*[VMEM] * len(kept)],
        out_specs=VMEM,
        compiler_params=limits(2),
    )(*[resident(value) for value in kept])


def body(inputs, w_input, w_recur, bias, h_start, c_start):
    steps, _, _ = inputs.shape
    unit = w_input.shape[3]
    layers = lax.axis_size("layer")
    devices = lax.axis_size("col")
    chips = devices // 2
    turns = steps + layers - 1
    same_core = [[2 * chip + side for chip in range(chips)] for side in range(2)]
    partners = [(i, i ^ 1) for i in range(devices)]
    upward = [(i, i + 1) for i in range(layers - 1)]

    def across(x):
        return lax.ppermute(x, "col", partners)

    def gathered(parts, stage):
        copies = spread(parts, stage, chips)
        return lax.all_to_all(copies, "col", 0, 0, tiled=True, axis_index_groups=same_core)

    cell = c_start[0]
    hidden = h_start[0]
    start = gathered((hidden,), 0)
    rec_send = across(sorted_side(w_recur[0], chips, True))
    in_send = across(sorted_side(w_input[0], chips, True))
    rec_keep = sorted_side(w_recur[0], chips, False)
    in_keep = sorted_side(w_input[0], chips, False)
    x = picked(inputs, chips, unit)
    rec_send, in_send, rec_keep, in_keep = fetched((rec_send, in_send, rec_keep, in_keep), start)

    kept = []
    blocks = (start,)
    for turn in range(turns):
        stage = min(turn, 2)
        fed = x if turn < steps else None
        came = across(product(blocks, fed, rec_send, in_send, turn, stage))
        here = product(blocks, fed, rec_keep, in_keep, turn, stage)
        cell, hidden = gates(here, came, bias[0], cell, hidden, turn, steps)
        kept.append(hidden)
        if turn + 1 < turns:
            below = lax.ppermute(hidden, "layer", upward)
            blocks = (gathered((hidden, below), min(turn + 1, 2)),)
            if turn == 0:
                blocks = (start, *blocks)
    return selected(kept, steps, layers)[None], cell[None]


def solution(mesh):
    in_specs = (
        P(),
        P("layer", None, None, "col"),
        P("layer", None, None, "col"),
        P("layer", None, "col"),
        P("layer", None, "col"),
        P("layer", None, "col"),
    )
    out_specs = (P("layer", None, None, "col"), P("layer", None, "col"))
    return jax.shard_map(body, mesh=mesh, in_specs=in_specs, out_specs=out_specs, check_vma=False)
```

```python
import functools

import jax
import jax.numpy as jnp
from jax import lax
from jax.experimental import pallas as pl
from jax.experimental.pallas import tpu as pltpu
from jax.sharding import PartitionSpec as P

VMEM = pl.BlockSpec(memory_space=pltpu.VMEM)
HBM = pl.BlockSpec(memory_space=pltpu.HBM)


def resident(x):
    return pltpu.with_memory_space_constraint(x, pltpu.VMEM)


def outside(x):
    return pltpu.with_memory_space_constraint(x, pltpu.HBM)


def limits(mib):
    return pltpu.CompilerParams(vmem_limit_bytes=mib << 20)


def own_side():
    return (lax.axis_index("col") & 1) == 0


def sort_kernel(away, in_ref, rec_ref, out_ref, natural, ordered, in_sems, out_sems):
    blocks, depth, wide = ordered.shape
    unit = natural.shape[2]
    gates = wide // unit
    rows = 2 * unit
    span = rows // gates
    to = lax.broadcasted_iota(jnp.int32, (rows, rows), 0)
    come = lax.broadcasted_iota(jnp.int32, (rows, rows), 1)
    order = come == gates * (to % span) + to // span
    order = order.astype(jnp.float32).astype(jnp.bfloat16)
    parts = in_sems.shape[0]
    size = blocks // parts
    from_input = own_side() if away else jnp.logical_not(own_side())

    def incoming(w_ref, part):
        chosen = pl.ds(part * size, size)
        return pltpu.make_async_copy(w_ref.at[chosen], natural.at[chosen], in_sems.at[part])

    def outgoing(part):
        chosen = pl.ds(part * size, size)
        return pltpu.make_async_copy(ordered.at[chosen], out_ref.at[chosen], out_sems.at[part])

    @pl.when(from_input)
    def _():
        for part in range(parts):
            incoming(in_ref, part).start()

    @pl.when(jnp.logical_not(from_input))
    def _():
        for part in range(parts):
            incoming(rec_ref, part).start()

    for part in range(parts):
        incoming(in_ref, part).wait()
        for j in range(part * size, (part + 1) * size):
            for q in range(0, depth // span, 2):
                both = jnp.concatenate(
                    [natural[j, (q + h) * rows : (q + h + 1) * rows, :] for h in range(2)], axis=1
                )
                moved = jnp.dot(order, both, preferred_element_type=jnp.float32)
                moved = moved.astype(jnp.bfloat16)
                for h in range(2):
                    at = (q + h) * span
                    for g in range(gates):
                        ordered[j, at : at + span, g * unit : (g + 1) * unit] = moved[
                            g * span : (g + 1) * span, h * unit : (h + 1) * unit
                        ]
        outgoing(part).start()
    for part in range(parts):
        outgoing(part).wait()


def sorted_weights(w_in, w_rec, blocks, away):
    gates, unit = w_in.shape[1:]
    depth = w_in.shape[0] // blocks
    wide = gates * unit
    parts = 4
    flat = (blocks, depth * gates, unit)
    return pl.pallas_call(
        functools.partial(sort_kernel, away),
        out_shape=pltpu.HBM((blocks, depth, wide), w_in.dtype),
        in_specs=[HBM, HBM],
        out_specs=HBM,
        scratch_shapes=[
            pltpu.VMEM(flat, w_in.dtype),
            pltpu.VMEM((blocks, depth, wide), w_in.dtype),
            pltpu.SemaphoreType.DMA((parts,)),
            pltpu.SemaphoreType.DMA((parts,)),
        ],
        cost_estimate=pl.CostEstimate(
            flops=4_000_000_000, bytes_accessed=4 * blocks * depth * wide, transcendentals=0
        ),
        compiler_params=limits(10),
    )(outside(w_in.reshape(flat)), outside(w_rec.reshape(flat)))


def fetch_kernel(count, *refs):
    sems = refs[-1]
    copies = [
        pltpu.make_async_copy(refs[i], refs[count + 1 + i], sems.at[i]) for i in range(count)
    ]
    for copy in copies:
        copy.start()
    for copy in copies:
        copy.wait()


def fetched(arrays, after):
    count = len(arrays)
    return pl.pallas_call(
        functools.partial(fetch_kernel, count),
        out_shape=tuple(jax.ShapeDtypeStruct(array.shape, array.dtype) for array in arrays),
        in_specs=[*[HBM] * count, pl.BlockSpec(memory_space=pl.ANY)],
        out_specs=tuple([VMEM] * count),
        scratch_shapes=[pltpu.SemaphoreType.DMA((count,))],
        compiler_params=limits(1),
    )(*[outside(array) for array in arrays], after)


def product_kernel(turn, fed, *refs):
    refs = list(refs)
    out_ref, w_ref = refs.pop(), refs.pop()
    x_ref = refs.pop() if fed else None
    blocks, depth, width = w_ref.shape
    bottom = jnp.logical_and(lax.axis_index("layer") == 0, jnp.logical_not(own_side()))

    def left(j):
        if len(refs) == 2:
            came = jnp.concatenate([refs[0][j], refs[1][j]], axis=1)
        else:
            came = refs[0][j]
        if fed:
            came = jnp.where(bottom, x_ref[turn, :, j * depth : (j + 1) * depth], came)
        return came

    wide = 256
    for n in range(width // wide):
        cols = slice(n * wide, (n + 1) * wide)
        total = None
        for j in range(blocks):
            term = jnp.dot(left(j), w_ref[j, :, cols], preferred_element_type=jnp.float32)
            total = term if total is None else total + term
        out_ref[:, cols] = total


def product(gathered, x, w, turn):
    blocks, depth, width = w.shape
    batch = gathered[0].shape[1]
    args = [*gathered, *([] if x is None else [x]), w]
    return pl.pallas_call(
        functools.partial(product_kernel, turn, x is not None),
        out_shape=jax.ShapeDtypeStruct((batch, width), jnp.float32),
        in_specs=[VMEM] * len(args),
        out_specs=VMEM,
        cost_estimate=pl.CostEstimate(
            flops=2 * blocks * depth * batch * width,
            bytes_accessed=2 * blocks * depth * (batch + width) + 4 * batch * width,
            transcendentals=0,
        ),
        compiler_params=limits(2),
    )(*[resident(arg) for arg in args])


def gates_kernel(turn, steps, layers, here_ref, came_ref, bias_ref, cell_ref, hid_ref, *refs):
    kept, (cell_out, hid_out) = refs[:-2], refs[-2:]
    unit = cell_ref.shape[1]
    layer = lax.axis_index("layer")
    valid = jnp.logical_and(turn >= layer, turn < layer + steps)

    def gate(k):
        cols = slice(k * unit, (k + 1) * unit)
        return here_ref[:, cols] + came_ref[:, cols] + bias_ref[k : k + 1, :]

    cell = cell_ref[...]
    cell_new = jax.nn.sigmoid(gate(1)) * cell + jax.nn.sigmoid(gate(0)) * jnp.tanh(gate(2))
    hidden_new = (jax.nn.sigmoid(gate(3)) * jnp.tanh(cell_new)).astype(hid_ref.dtype)
    hidden_new = jnp.where(valid, hidden_new, hid_ref[...])
    cell_out[...] = jnp.where(valid, cell_new, cell)
    if not kept:
        hid_out[...] = hidden_new
        return
    states = [*[ref[...] for ref in kept], hidden_new]
    for t in range(steps):
        value = states[t]
        for l in range(1, layers):
            value = jnp.where(layer == l, states[t + l], value)
        hid_out[t] = value


def gates(here, came, bias, cell, hidden, turn, steps, layers, kept=()):
    hid_shape = (steps, *hidden.shape) if kept else hidden.shape
    args = (here, came, bias, cell, hidden, *kept)
    return pl.pallas_call(
        functools.partial(gates_kernel, turn, steps, layers),
        out_shape=(
            jax.ShapeDtypeStruct(cell.shape, cell.dtype),
            jax.ShapeDtypeStruct(hid_shape, hidden.dtype),
        ),
        in_specs=[VMEM] * len(args),
        out_specs=(VMEM, VMEM),
        cost_estimate=pl.CostEstimate(
            flops=20 * cell.size, bytes_accessed=40 * cell.size, transcendentals=5 * cell.size
        ),
        compiler_params=limits(2),
    )(*[resident(arg) for arg in args])


def spread_kernel(*refs):
    out_ref = refs[-1]
    if len(refs) == 2:
        block = refs[0][...]
    else:
        hidden, first, second = (ref[...] for ref in refs[:3])
        block = jnp.concatenate(
            [jnp.where(own_side(), hidden, first), jnp.where(own_side(), first, second)], axis=1
        )
    for j in range(out_ref.shape[0]):
        out_ref[j] = block


def spread(parts, copies):
    batch, unit = parts[0].shape
    width = unit * (1 if len(parts) == 1 else 2)
    return pl.pallas_call(
        spread_kernel,
        out_shape=jax.ShapeDtypeStruct((copies, batch, width), parts[0].dtype),
        in_specs=[VMEM] * len(parts),
        out_specs=VMEM,
        cost_estimate=pl.CostEstimate(
            flops=batch * width, bytes_accessed=2 * copies * batch * width, transcendentals=0
        ),
        compiler_params=limits(2),
    )(*[resident(part) for part in parts])


def body(inputs, w_input, w_recur, bias, h_start, c_start):
    steps = inputs.shape[0]
    layers = lax.axis_size("layer")
    devices = lax.axis_size("col")
    chips = devices // 2
    turns = steps + layers - 1
    same_core = [[2 * chip + side for chip in range(chips)] for side in range(2)]
    partners = [(i, i ^ 1) for i in range(devices)]
    chip_bases = [(l, l * devices + 2 * chip) for l in range(layers) for chip in range(chips)]
    beside = [(base + 1, base) for _, base in chip_bases]
    upward = [(base, base + devices + 1) for l, base in chip_bases if l + 1 < layers]
    upward_too = [(base + 1, base + devices + 1) for l, base in chip_bases if l + 1 < layers]

    def across(x):
        return lax.ppermute(x, "col", partners)

    def gathered(*parts):
        copies = spread(parts, chips)
        return lax.all_to_all(copies, "col", 0, 0, tiled=True, axis_index_groups=same_core)

    cell = c_start[0]
    hidden = h_start[0]
    start = gathered(hidden)
    given = across(sorted_weights(w_input[0], w_recur[0], chips, True))
    w_here = sorted_weights(w_input[0], w_recur[0], chips, False)
    (w_there,) = fetched((given,), start)

    kept = []
    blocks = (start, across(start))
    for turn in range(turns):
        fed = inputs if turn < steps else None
        came = across(product(blocks, fed, w_there, turn))
        here = product(blocks, fed, w_here, turn)
        last = tuple(kept) if turn + 1 == turns else ()
        cell, hidden = gates(here, came, bias[0], cell, hidden, turn, steps, layers, last)
        kept.append(hidden)
        if turn + 1 < turns:
            first = lax.ppermute(hidden, ("layer", "col"), beside + upward)
            second = lax.ppermute(hidden, ("layer", "col"), upward_too)
            blocks = (gathered(hidden, first, second),)
    return hidden[None], cell[None]


def solution(mesh):
    in_specs = (
        P(),
        P("layer", None, None, "col"),
        P("layer", None, None, "col"),
        P("layer", None, "col"),
        P("layer", None, "col"),
        P("layer", None, "col"),
    )
    out_specs = (P("layer", None, None, "col"), P("layer", None, "col"))
    return jax.shard_map(body, mesh=mesh, in_specs=in_specs, out_specs=out_specs, check_vma=False)
```

```python
import functools

import jax
import jax.numpy as jnp
from jax import lax
from jax.experimental import pallas as pl
from jax.experimental.pallas import tpu as pltpu
from jax.sharding import PartitionSpec as P

VMEM = pl.BlockSpec(memory_space=pltpu.VMEM)
HBM = pl.BlockSpec(memory_space=pltpu.HBM)


def resident(x):
    return pltpu.with_memory_space_constraint(x, pltpu.VMEM)


def outside(x):
    return pltpu.with_memory_space_constraint(x, pltpu.HBM)


def limits(mib):
    return pltpu.CompilerParams(vmem_limit_bytes=mib << 20)


def sort_kernel(w_ref, keep_ref, away_ref, natural, ordered, in_sems, out_sems):
    blocks, _, depth, wide = ordered.shape
    unit = natural.shape[3]
    gates = wide // unit
    half = depth // 2
    rows = half * gates
    core = lax.axis_index("col") & 1
    to = lax.broadcasted_iota(jnp.int32, (rows, rows), 0)
    come = lax.broadcasted_iota(jnp.int32, (rows, rows), 1)
    order = come == gates * (to % half) + to // half
    order = order.astype(jnp.float32).astype(jnp.bfloat16)
    parts = in_sems.shape[0]
    size = blocks // parts

    def incoming(part):
        chosen = pl.ds(part * size, size)
        return pltpu.make_async_copy(w_ref.at[chosen], natural.at[chosen], in_sems.at[part])

    def outgoing(part, away):
        chosen = pl.ds(part * size, size)
        side = 1 - core if away else core
        return pltpu.make_async_copy(
            ordered.at[chosen, side],
            (away_ref if away else keep_ref).at[chosen],
            out_sems.at[part, away],
        )

    for part in range(parts):
        incoming(part).start()
    for part in range(parts):
        incoming(part).wait()
        for j in range(part * size, (part + 1) * size):
            for side in range(2):
                both = jnp.concatenate(
                    [natural[j, side, :rows, :], natural[j, side, rows:, :]], axis=1
                )
                moved = jnp.dot(order, both, preferred_element_type=jnp.float32)
                moved = moved.astype(jnp.bfloat16)
                for h in range(2):
                    for g in range(gates):
                        ordered[j, side, h * half : (h + 1) * half, g * unit : (g + 1) * unit] = (
                            moved[g * half : (g + 1) * half, h * unit : (h + 1) * unit]
                        )
        for away in range(2):
            outgoing(part, away).start()
    for part in range(parts):
        for away in range(2):
            outgoing(part, away).wait()


def sorted_weights(w, blocks):
    gates, unit = w.shape[1:]
    depth = w.shape[0] // (2 * blocks)
    wide = gates * unit
    parts = 4
    return pl.pallas_call(
        sort_kernel,
        out_shape=tuple([pltpu.HBM((blocks, depth, wide), w.dtype)] * 2),
        in_specs=[HBM],
        out_specs=(HBM, HBM),
        scratch_shapes=[
            pltpu.VMEM((blocks, 2, depth * gates, unit), w.dtype),
            pltpu.VMEM((blocks, 2, depth, wide), w.dtype),
            pltpu.SemaphoreType.DMA((parts,)),
            pltpu.SemaphoreType.DMA((parts, 2)),
        ],
        cost_estimate=pl.CostEstimate(
            flops=4_000_000_000, bytes_accessed=8 * blocks * depth * wide, transcendentals=0
        ),
        compiler_params=limits(10),
    )(outside(w.reshape(blocks, 2, depth * gates, unit)))


def block_of(x_ref, turn, j, side, unit):
    at = pl.multiple_of((2 * j + side) * unit, unit)
    return x_ref[turn, :, pl.ds(at, unit)]


def first_kernel(own_ref, other_ref, x_ref, *refs):
    weights, (out_ref, *kept), (*away, x_held, sems, x_sem) = refs[:4], refs[4:7], refs[7:]
    blocks, unit, width = kept[0].shape
    core = lax.axis_index("col") & 1
    parts = sems.shape[1]
    size = blocks // parts
    places = (*kept, *away)

    def incoming(i, part):
        chosen = pl.ds(part * size, size)
        return pltpu.make_async_copy(
            weights[i].at[chosen], places[i].at[chosen], sems.at[i, part]
        )

    def left(i, j):
        if i == 0:
            return own_ref[j]
        if i == 2:
            return other_ref[j]
        return block_of(x_held, 0, j, core if i == 1 else 1 - core, unit)

    x_copy = pltpu.make_async_copy(x_ref.at[pl.ds(0, 1)], x_held, x_sem)
    for i in range(4):
        for part in range(parts):
            incoming(i, part).start()
        if i == 0:
            x_copy.start()
    wide = 256
    for i in range(4):
        if i == 1:
            x_copy.wait()
        for part in range(parts):
            incoming(i, part).wait()
            for n in range(width // wide):
                cols = slice(n * wide, (n + 1) * wide)
                total = None if i + part == 0 else out_ref[:, cols]
                for j in range(part * size, (part + 1) * size, 2):
                    pair = jnp.concatenate([left(i, j), left(i, j + 1)], axis=1)
                    right = places[i][j : j + 2, :, cols].reshape(2 * unit, wide)
                    term = jnp.dot(pair, right, preferred_element_type=jnp.float32)
                    total = term if total is None else total + term
                out_ref[:, cols] = total


def first_product(own, other, x, keeps, aways):
    blocks, unit, width = keeps[0].shape
    batch = own.shape[1]
    held = jax.ShapeDtypeStruct(keeps[0].shape, keeps[0].dtype)
    parts = 2
    return pl.pallas_call(
        first_kernel,
        out_shape=(jax.ShapeDtypeStruct((batch, width), jnp.float32), held, held),
        in_specs=[*[VMEM] * 2, *[HBM] * 5],
        out_specs=(VMEM, VMEM, VMEM),
        scratch_shapes=[
            pltpu.VMEM(keeps[0].shape, keeps[0].dtype),
            pltpu.VMEM(keeps[0].shape, keeps[0].dtype),
            pltpu.VMEM((1, *x.shape[1:]), x.dtype),
            pltpu.SemaphoreType.DMA((4, parts)),
            pltpu.SemaphoreType.DMA,
        ],
        cost_estimate=pl.CostEstimate(
            flops=8 * blocks * unit * batch * width,
            bytes_accessed=8 * blocks * unit * width,
            transcendentals=0,
        ),
        compiler_params=limits(7),
    )(resident(own), resident(other), *[outside(value) for value in (x, *keeps, *aways)])


def product_kernel(turn, stage, fed, *refs):
    refs = list(refs)
    out_ref, w_in_ref, w_rec_ref = refs.pop(), refs.pop(), refs.pop()
    x_ref = refs.pop() if fed else None
    blocks, unit, width = w_rec_ref.shape
    bottom = lax.axis_index("layer") == 0
    core = lax.axis_index("col") & 1

    def own(j):
        if stage == 1:
            return jnp.where(bottom, refs[1][j], refs[0][j])
        return refs[0][j, :, :unit]

    def below(j):
        came = refs[1][j] if stage == 1 else refs[0][j, :, unit:]
        return jnp.where(bottom, block_of(x_ref, turn, j, core, unit), came) if fed else came

    wide = 256
    for n in range(width // wide):
        cols = slice(n * wide, (n + 1) * wide)
        total = None
        for block, w_ref in ((own, w_rec_ref), (below, w_in_ref)):
            for j in range(0, blocks, 2):
                left = jnp.concatenate([block(j), block(j + 1)], axis=1)
                right = w_ref[j : j + 2, :, cols].reshape(2 * unit, wide)
                term = jnp.dot(left, right, preferred_element_type=jnp.float32)
                total = term if total is None else total + term
        out_ref[:, cols] = total


def product(gathered, x, w_rec, w_in, turn, stage):
    blocks, unit, width = w_rec.shape
    batch = gathered[0].shape[1]
    args = [*gathered, *([] if x is None else [x]), w_rec, w_in]
    return pl.pallas_call(
        functools.partial(product_kernel, turn, stage, x is not None),
        out_shape=jax.ShapeDtypeStruct((batch, width), jnp.float32),
        in_specs=[*[VMEM] * len(args)],
        out_specs=VMEM,
        cost_estimate=pl.CostEstimate(
            flops=4 * blocks * unit * batch * width,
            bytes_accessed=4 * blocks * unit * (batch + width) + 4 * batch * width,
            transcendentals=0,
        ),
        compiler_params=limits(4),
    )(*[resident(arg) for arg in args])


def gates_kernel(turn, steps, layers, parts, *refs):
    sums, (bias_ref, cell_ref, hid_ref) = refs[:parts], refs[parts : parts + 3]
    kept, (cell_out, hid_out) = refs[parts + 3 : -2], refs[-2:]
    unit = cell_ref.shape[1]
    layer = lax.axis_index("layer")
    valid = jnp.logical_and(turn >= layer, turn < layer + steps)

    def gate(k):
        cols = slice(k * unit, (k + 1) * unit)
        total = bias_ref[k : k + 1, :]
        for ref in sums:
            total = total + ref[:, cols]
        return total

    cell = cell_ref[...]
    cell_new = jax.nn.sigmoid(gate(1)) * cell + jax.nn.sigmoid(gate(0)) * jnp.tanh(gate(2))
    hidden_new = (jax.nn.sigmoid(gate(3)) * jnp.tanh(cell_new)).astype(hid_ref.dtype)
    hidden_new = jnp.where(valid, hidden_new, hid_ref[...])
    cell_out[...] = jnp.where(valid, cell_new, cell)
    if not kept:
        hid_out[...] = hidden_new
        return
    states = [*[ref[...] for ref in kept], hidden_new]
    for t in range(steps):
        value = states[t]
        for l in range(1, layers):
            value = jnp.where(layer == l, states[t + l], value)
        hid_out[t] = value


def gates(sums, bias, cell, hidden, turn, steps, layers, kept=()):
    hid_shape = (steps, *hidden.shape) if kept else hidden.shape
    args = (*sums, bias, cell, hidden, *kept)
    return pl.pallas_call(
        functools.partial(gates_kernel, turn, steps, layers, len(sums)),
        out_shape=(
            jax.ShapeDtypeStruct(cell.shape, cell.dtype),
            jax.ShapeDtypeStruct(hid_shape, hidden.dtype),
        ),
        in_specs=[VMEM] * len(args),
        out_specs=(VMEM, VMEM),
        cost_estimate=pl.CostEstimate(
            flops=20 * cell.size, bytes_accessed=40 * cell.size, transcendentals=5 * cell.size
        ),
        compiler_params=limits(2),
    )(*[resident(arg) for arg in args])


def spread_kernel(stage, *refs):
    out_ref = refs[-1]
    unit = refs[0].shape[1]
    layer = lax.axis_index("layer")
    for j in range(out_ref.shape[0]):
        if stage == 0:
            out_ref[j] = refs[0][...]
        elif stage == 1:
            out_ref[j] = jnp.where(layer == 0, refs[0][...], refs[1][...])
        else:
            out_ref[j, :, :unit] = refs[0][...]
            out_ref[j, :, unit:] = refs[1][...]


def spread(parts, stage, copies):
    batch, unit = parts[0].shape
    width = unit * (2 if stage == 2 else 1)
    return pl.pallas_call(
        functools.partial(spread_kernel, stage),
        out_shape=jax.ShapeDtypeStruct((copies, batch, width), parts[0].dtype),
        in_specs=[*[VMEM] * len(parts)],
        out_specs=VMEM,
        cost_estimate=pl.CostEstimate(
            flops=batch * width, bytes_accessed=2 * copies * batch * width, transcendentals=0
        ),
        compiler_params=limits(2),
    )(*[resident(part) for part in parts])


def body(inputs, w_input, w_recur, bias, h_start, c_start):
    steps, _, _ = inputs.shape
    layers = lax.axis_size("layer")
    devices = lax.axis_size("col")
    chips = devices // 2
    turns = steps + layers - 1
    same_core = [[2 * chip + side for chip in range(chips)] for side in range(2)]
    partners = [(i, i ^ 1) for i in range(devices)]
    upward = [(i, (i + 1) % layers) for i in range(layers)]

    def across(x):
        return lax.ppermute(x, "col", partners)

    def gathered(parts, stage):
        copies = spread(parts, stage, chips)
        return lax.all_to_all(copies, "col", 0, 0, tiled=True, axis_index_groups=same_core)

    cell = c_start[0]
    hidden = h_start[0]
    start = gathered((hidden,), 0)
    rec_keep, rec_away = sorted_weights(w_recur[0], chips)
    in_keep, in_away = sorted_weights(w_input[0], chips)
    other = across(start)
    *leaving, other = lax.optimization_barrier((rec_away, in_away, other))
    rec_send, in_send = (across(away) for away in leaving)

    kept = []
    for turn in range(turns):
        fed = inputs if turn < steps else None
        if turn == 0:
            z, rec_keep, in_keep = first_product(
                start, other, fed, (rec_keep, in_keep), (rec_away, in_away)
            )
            sums = (z,)
        else:
            stage = min(turn, 2)
            came = across(product(blocks, fed, rec_send, in_send, turn, stage))
            sums = (product(blocks, fed, rec_keep, in_keep, turn, stage), came)
        last = tuple(kept) if turn + 1 == turns else ()
        cell, hidden = gates(sums, bias[0], cell, hidden, turn, steps, layers, last)
        kept.append(hidden)
        if turn + 1 < turns:
            below = lax.ppermute(hidden, "layer", upward)
            blocks = (gathered((hidden, below), min(turn + 1, 2)),)
            if turn == 0:
                blocks = (start, *blocks)
    return hidden[None], cell[None]


def solution(mesh):
    in_specs = (
        P(),
        P("layer", None, None, "col"),
        P("layer", None, None, "col"),
        P("layer", None, "col"),
        P("layer", None, "col"),
        P("layer", None, "col"),
    )
    out_specs = (P("layer", None, None, "col"), P("layer", None, "col"))
    return jax.shard_map(body, mesh=mesh, in_specs=in_specs, out_specs=out_specs, check_vma=False)
```

```python
import functools

import jax
import jax.numpy as jnp
from jax import lax
from jax.experimental import pallas as pl
from jax.experimental.pallas import tpu as pltpu
from jax.sharding import PartitionSpec as P

VMEM = pl.BlockSpec(memory_space=pltpu.VMEM)
HBM = pl.BlockSpec(memory_space=pltpu.HBM)


def resident(x):
    return pltpu.with_memory_space_constraint(x, pltpu.VMEM)


def outside(x):
    return pltpu.with_memory_space_constraint(x, pltpu.HBM)


def limits(mib):
    return pltpu.CompilerParams(vmem_limit_bytes=mib << 20)


def sort_kernel(fed, *refs):
    refs = list(refs)
    w_ref = refs.pop(0)
    x_ref = refs.pop(0) if fed else None
    keep_ref, away_ref = refs.pop(0), refs.pop(0)
    sum_ref = refs.pop(0) if fed else None
    natural, ordered, in_sems, out_sems = refs[:4]
    blocks, _, depth, wide = ordered.shape
    unit = natural.shape[3]
    gates = wide // unit
    half = depth // 2
    rows = half * gates
    core = lax.axis_index("col") & 1
    to = lax.broadcasted_iota(jnp.int32, (rows, rows), 0)
    come = lax.broadcasted_iota(jnp.int32, (rows, rows), 1)
    order = come == gates * (to % half) + to // half
    order = order.astype(jnp.float32).astype(jnp.bfloat16)
    parts = in_sems.shape[0]
    size = blocks // parts

    def incoming(part):
        chosen = pl.ds(part * size, size)
        return pltpu.make_async_copy(w_ref.at[chosen], natural.at[chosen], in_sems.at[part])

    def outgoing(part, away):
        chosen = pl.ds(part * size, size)
        side = 1 - core if away else core
        return pltpu.make_async_copy(
            ordered.at[chosen, side],
            (away_ref if away else keep_ref).at[chosen],
            out_sems.at[part, away],
        )

    for part in range(parts):
        incoming(part).start()
        if fed and part == 0:
            x_held, x_sem = refs[4:]
            x_copy = pltpu.make_async_copy(x_ref.at[0], x_held, x_sem)
            x_copy.start()
    for part in range(parts):
        incoming(part).wait()
        for j in range(part * size, (part + 1) * size):
            for side in range(2):
                both = jnp.concatenate(
                    [natural[j, side, :rows, :], natural[j, side, rows:, :]], axis=1
                )
                moved = jnp.dot(order, both, preferred_element_type=jnp.float32)
                moved = moved.astype(jnp.bfloat16)
                for h in range(2):
                    for g in range(gates):
                        ordered[j, side, h * half : (h + 1) * half, g * unit : (g + 1) * unit] = (
                            moved[g * half : (g + 1) * half, h * unit : (h + 1) * unit]
                        )
        for away in range(2):
            outgoing(part, away).start()
        if fed:
            if part == 0:
                x_copy.wait()
            for cols in (slice(n, n + 256) for n in range(0, wide, 256)):
                total = None if part == 0 else sum_ref[:, cols]
                for j in range(part * size, (part + 1) * size):
                    left = x_held[:, 2 * j * depth : 2 * (j + 1) * depth]
                    right = ordered[j, :, :, cols].reshape(2 * depth, 256)
                    term = jnp.dot(left, right, preferred_element_type=jnp.float32)
                    total = term if total is None else total + term
                sum_ref[:, cols] = total
    for part in range(parts):
        for away in range(2):
            outgoing(part, away).wait()


def sorted_weights(w, blocks, x=None):
    gates, unit = w.shape[1:]
    depth = w.shape[0] // (2 * blocks)
    wide = gates * unit
    parts = 4
    fed = x is not None
    sides = [pltpu.HBM((blocks, depth, wide), w.dtype)] * 2
    natural = (blocks, 2, depth * gates, unit)
    return pl.pallas_call(
        functools.partial(sort_kernel, fed),
        out_shape=(*sides, *([jax.ShapeDtypeStruct((x.shape[1], wide), jnp.float32)] if fed else [])),
        in_specs=[HBM] * (1 + fed),
        out_specs=(HBM, HBM, *([VMEM] if fed else [])),
        scratch_shapes=[
            pltpu.VMEM(natural, w.dtype),
            pltpu.VMEM((blocks, 2, depth, wide), w.dtype),
            pltpu.SemaphoreType.DMA((parts,)),
            pltpu.SemaphoreType.DMA((parts, 2)),
            *([pltpu.VMEM(x.shape[1:], x.dtype), pltpu.SemaphoreType.DMA] if fed else []),
        ],
        cost_estimate=pl.CostEstimate(
            flops=4_000_000_000, bytes_accessed=8 * blocks * depth * wide, transcendentals=0
        ),
        compiler_params=limits(12),
    )(outside(w.reshape(natural)), *([outside(x)] if fed else []))


def block_of(x_ref, turn, j, side, unit):
    at = pl.multiple_of((2 * j + side) * unit, unit)
    return x_ref[turn, :, pl.ds(at, unit)]


def first_kernel(acc_ref, own_ref, keep_ref, away_ref, out_ref, kept_ref, held_ref, sems):
    blocks, unit, width = kept_ref.shape
    parts = sems.shape[1]
    size = blocks // parts

    def incoming(away, part):
        chosen = pl.ds(part * size, size)
        from_ref, to_ref = (away_ref, held_ref) if away else (keep_ref, kept_ref)
        return pltpu.make_async_copy(from_ref.at[chosen], to_ref.at[chosen], sems.at[away, part])

    for away in range(2):
        for part in range(parts):
            incoming(away, part).start()
    wide = 256
    for part in range(parts):
        incoming(0, part).wait()
        for n in range(width // wide):
            cols = slice(n * wide, (n + 1) * wide)
            total = out_ref[:, cols] if part else acc_ref[:, cols]
            for j in range(part * size, (part + 1) * size, 2):
                pair = jnp.concatenate([own_ref[j], own_ref[j + 1]], axis=1)
                right = kept_ref[j : j + 2, :, cols].reshape(2 * unit, wide)
                total = total + jnp.dot(pair, right, preferred_element_type=jnp.float32)
            out_ref[:, cols] = total
    for part in range(parts):
        incoming(1, part).wait()


def first_product(acc, own, keep, away):
    blocks, unit, width = keep.shape
    held = jax.ShapeDtypeStruct(keep.shape, keep.dtype)
    parts = 2
    return pl.pallas_call(
        first_kernel,
        out_shape=(jax.ShapeDtypeStruct(acc.shape, acc.dtype), held, held),
        in_specs=[VMEM, VMEM, HBM, HBM],
        out_specs=(VMEM, VMEM, VMEM),
        scratch_shapes=[pltpu.SemaphoreType.DMA((2, parts))],
        cost_estimate=pl.CostEstimate(
            flops=2 * blocks * unit * acc.shape[0] * width,
            bytes_accessed=4 * blocks * unit * width,
            transcendentals=0,
        ),
        compiler_params=limits(2),
    )(resident(acc), resident(own), outside(keep), outside(away))


def added_kernel(acc_ref, g_ref, w_ref, out_ref):
    blocks, unit, width = w_ref.shape
    wide = 256
    for n in range(width // wide):
        cols = slice(n * wide, (n + 1) * wide)
        total = acc_ref[:, cols]
        for j in range(0, blocks, 2):
            pair = jnp.concatenate([g_ref[j], g_ref[j + 1]], axis=1)
            right = w_ref[j : j + 2, :, cols].reshape(2 * unit, wide)
            total = total + jnp.dot(pair, right, preferred_element_type=jnp.float32)
        out_ref[:, cols] = total


def added_product(acc, g, w):
    blocks, unit, width = w.shape
    return pl.pallas_call(
        added_kernel,
        out_shape=jax.ShapeDtypeStruct(acc.shape, acc.dtype),
        in_specs=[VMEM] * 3,
        out_specs=VMEM,
        cost_estimate=pl.CostEstimate(
            flops=2 * blocks * unit * width * acc.shape[0],
            bytes_accessed=2 * blocks * unit * width,
            transcendentals=0,
        ),
        compiler_params=limits(2),
    )(*[resident(value) for value in (acc, g, w)])


def product_kernel(turn, stage, fed, *refs):
    refs = list(refs)
    out_ref, w_in_ref, w_rec_ref = refs.pop(), refs.pop(), refs.pop()
    x_ref = refs.pop() if fed else None
    blocks, unit, width = w_rec_ref.shape
    bottom = lax.axis_index("layer") == 0
    core = lax.axis_index("col") & 1

    def own(j):
        if stage == 1:
            return jnp.where(bottom, refs[1][j], refs[0][j])
        return refs[0][j, :, :unit]

    def below(j):
        came = refs[1][j] if stage == 1 else refs[0][j, :, unit:]
        return jnp.where(bottom, block_of(x_ref, turn, j, core, unit), came) if fed else came

    wide = 256
    for n in range(width // wide):
        cols = slice(n * wide, (n + 1) * wide)
        total = None
        for block, w_ref in ((own, w_rec_ref), (below, w_in_ref)):
            for j in range(0, blocks, 2):
                left = jnp.concatenate([block(j), block(j + 1)], axis=1)
                right = w_ref[j : j + 2, :, cols].reshape(2 * unit, wide)
                term = jnp.dot(left, right, preferred_element_type=jnp.float32)
                total = term if total is None else total + term
        out_ref[:, cols] = total


def product(gathered, x, w_rec, w_in, turn, stage):
    blocks, unit, width = w_rec.shape
    batch = gathered[0].shape[1]
    args = [*gathered, *([] if x is None else [x]), w_rec, w_in]
    return pl.pallas_call(
        functools.partial(product_kernel, turn, stage, x is not None),
        out_shape=jax.ShapeDtypeStruct((batch, width), jnp.float32),
        in_specs=[*[VMEM] * len(args)],
        out_specs=VMEM,
        cost_estimate=pl.CostEstimate(
            flops=4 * blocks * unit * batch * width,
            bytes_accessed=4 * blocks * unit * (batch + width) + 4 * batch * width,
            transcendentals=0,
        ),
        compiler_params=limits(4),
    )(*[resident(arg) for arg in args])


def gates_kernel(turn, steps, layers, parts, *refs):
    sums, (bias_ref, cell_ref, hid_ref) = refs[:parts], refs[parts : parts + 3]
    kept, (cell_out, hid_out) = refs[parts + 3 : -2], refs[-2:]
    unit = cell_ref.shape[1]
    layer = lax.axis_index("layer")
    valid = jnp.logical_and(turn >= layer, turn < layer + steps)

    def gate(k):
        cols = slice(k * unit, (k + 1) * unit)
        total = bias_ref[k : k + 1, :]
        for ref in sums:
            total = total + ref[:, cols]
        return total

    cell = cell_ref[...]
    cell_new = jax.nn.sigmoid(gate(1)) * cell + jax.nn.sigmoid(gate(0)) * jnp.tanh(gate(2))
    hidden_new = (jax.nn.sigmoid(gate(3)) * jnp.tanh(cell_new)).astype(hid_ref.dtype)
    hidden_new = jnp.where(valid, hidden_new, hid_ref[...])
    cell_out[...] = jnp.where(valid, cell_new, cell)
    if not kept:
        hid_out[...] = hidden_new
        return
    states = [*[ref[...] for ref in kept], hidden_new]
    for t in range(steps):
        value = states[t]
        for l in range(1, layers):
            value = jnp.where(layer == l, states[t + l], value)
        hid_out[t] = value


def gates(sums, bias, cell, hidden, turn, steps, layers, kept=()):
    hid_shape = (steps, *hidden.shape) if kept else hidden.shape
    args = (*sums, bias, cell, hidden, *kept)
    return pl.pallas_call(
        functools.partial(gates_kernel, turn, steps, layers, len(sums)),
        out_shape=(
            jax.ShapeDtypeStruct(cell.shape, cell.dtype),
            jax.ShapeDtypeStruct(hid_shape, hidden.dtype),
        ),
        in_specs=[VMEM] * len(args),
        out_specs=(VMEM, VMEM),
        cost_estimate=pl.CostEstimate(
            flops=20 * cell.size, bytes_accessed=40 * cell.size, transcendentals=5 * cell.size
        ),
        compiler_params=limits(2),
    )(*[resident(arg) for arg in args])


def spread_kernel(stage, *refs):
    out_ref = refs[-1]
    unit = refs[0].shape[1]
    layer = lax.axis_index("layer")
    for j in range(out_ref.shape[0]):
        if stage == 0:
            out_ref[j] = refs[0][...]
        elif stage == 1:
            out_ref[j] = jnp.where(layer == 0, refs[0][...], refs[1][...])
        else:
            out_ref[j, :, :unit] = refs[0][...]
            out_ref[j, :, unit:] = refs[1][...]


def spread(parts, stage, copies):
    batch, unit = parts[0].shape
    width = unit * (2 if stage == 2 else 1)
    return pl.pallas_call(
        functools.partial(spread_kernel, stage),
        out_shape=jax.ShapeDtypeStruct((copies, batch, width), parts[0].dtype),
        in_specs=[*[VMEM] * len(parts)],
        out_specs=VMEM,
        cost_estimate=pl.CostEstimate(
            flops=batch * width, bytes_accessed=2 * copies * batch * width, transcendentals=0
        ),
        compiler_params=limits(2),
    )(*[resident(part) for part in parts])


def body(inputs, w_input, w_recur, bias, h_start, c_start):
    steps, _, _ = inputs.shape
    layers = lax.axis_size("layer")
    devices = lax.axis_size("col")
    chips = devices // 2
    turns = steps + layers - 1
    same_core = [[2 * chip + side for chip in range(chips)] for side in range(2)]
    partners = [(i, i ^ 1) for i in range(devices)]
    upward = [(i, (i + 1) % layers) for i in range(layers)]

    def across(x):
        return lax.ppermute(x, "col", partners)

    def gathered(parts, stage):
        copies = spread(parts, stage, chips)
        return lax.all_to_all(copies, "col", 0, 0, tiled=True, axis_index_groups=same_core)

    cell = c_start[0]
    hidden = h_start[0]
    start = gathered((hidden,), 0)
    rec_keep, rec_away = sorted_weights(w_recur[0], chips)
    in_keep, in_away, z = sorted_weights(w_input[0], chips, inputs)
    other = across(start)
    z, rec_keep, rec_held = first_product(z, start, rec_keep, rec_away)
    rec_away, in_away, z = lax.optimization_barrier((rec_away, in_away, z))
    rec_send, in_send = across(rec_away), across(in_away)
    kept = []
    for turn in range(turns):
        fed = inputs if turn < steps else None
        if turn == 0:
            sums = (added_product(z, other, rec_held),)
        else:
            stage = min(turn, 2)
            came = across(product(blocks, fed, rec_send, in_send, turn, stage))
            sums = (product(blocks, fed, rec_keep, in_keep, turn, stage), came)
        last = tuple(kept) if turn + 1 == turns else ()
        cell, hidden = gates(sums, bias[0], cell, hidden, turn, steps, layers, last)
        kept.append(hidden)
        if turn + 1 < turns:
            below = lax.ppermute(hidden, "layer", upward)
            blocks = (gathered((hidden, below), min(turn + 1, 2)),)
            if turn == 0:
                blocks = (start, *blocks)
    return hidden[None], cell[None]


def solution(mesh):
    in_specs = (
        P(),
        P("layer", None, None, "col"),
        P("layer", None, None, "col"),
        P("layer", None, "col"),
        P("layer", None, "col"),
        P("layer", None, "col"),
    )
    out_specs = (P("layer", None, None, "col"), P("layer", None, "col"))
    return jax.shard_map(body, mesh=mesh, in_specs=in_specs, out_specs=out_specs, check_vma=False)
```
